32 devices in a mesh: dp: 8 (over z, y), mp: 4 (over x, core).
Axes of the slice: x: 2, y: 2, z: 4, core: 2. Of those that a mesh axis runs over, the one named last changes fastest.
Arguments:
- logits: bfloat16 [1024, 16384], P('dp', 'mp'), may hold values from -72 to 240
- targets: int32 [1024], P('dp'), may hold values from 0 to 16383
- resp_mask: int32 [1024], P('dp'), may hold values from 0 to 1, as said below
- rewards: int32 [8], P('dp'), may hold values from 0 to 10
- groups: int32 [8], P('dp'), may hold values from 0 to 1, as said below
- unit_grad: bfloat16 [1024, 8192], P(('dp', 'mp')), may hold values from -192 to 192
- mix: bfloat16 [1024, 2048], P('dp', 'mp'), may hold values from -6 to 6
- w_out: bfloat16 [2048, 8192], P('mp', 'dp'), may hold values from -0.125 to 0.125
Outputs:
- token_logprob: float32 [1024], P('dp')
- policy_loss: float32 [], replicated
- grad_mix: bfloat16 [1024, 2048], P('dp', 'mp')
- grad_w_out: bfloat16 [2048, 8192], P('mp', 'dp')
The draws below stay inside these ranges and needn't reach their ends.
Inputs may be any that keep to these rules, and one draw needn't show every extreme that they name: `resp_mask`: in each sample the response mask is a run of ones followed by zeros, with at least 32 ones. `groups`: each prompt id names exactly 4 samples.
All inputs are finite; a program needn't handle non-finite values.
Results may differ from the reference program's by a relative error of at most 0.005.
Values may be sent and summed in bfloat16 or wider, within the bound.
A program may use at most 64 MiB of HBM per device.

```python
import jax
import jax.numpy as jnp
from jax import lax

D = 8192
K = 4
ROWS = 128
SEQS = 8
PROMPTS = 2
TOKENS = 1024
VOCAB = 16384
QW = 2048


def draw_logits(key, part):
    keys = jax.random.split(key, 1)
    values = 3.0 * jnp.clip(jax.random.normal(keys[0], (TOKENS, VOCAB), jnp.float32), -6.0, 6.0)
    return values.astype(jnp.bfloat16)


def draw_resp_mask(key, part):
    jitter = jax.random.randint(key, (SEQS, 1), 0, ROWS // 8 + 1)
    sample_index = jnp.arange(SEQS, dtype=jnp.int32)[:, None]
    length = jnp.minimum(ROWS // 4 + sample_index * (ROWS * 3 // 4) // SEQS + jitter, ROWS)
    position = jnp.arange(ROWS, dtype=jnp.int32)[None, :]
    return (position < length).astype(jnp.int32).reshape(TOKENS)


def draw_groups(key, part):
    return (jax.random.permutation(key, SEQS) // K).astype(jnp.int32)


def touch_ends(values, key, least, top_value):
    extent = values.shape
    place = [jax.random.randint(jax.random.fold_in(key, axis), (), 0, extent[axis]) for axis in range(len(extent))]
    values = values.at[tuple(place)].set(least)
    longest = extent.index(max(extent))
    place[longest] = (place[longest] + 1) % extent[longest]
    return values.at[tuple(place)].set(top_value)


def block_scale(own_key, shape, pieces, least, high):
    def one(dim, blocks):
        draws = jax.random.uniform(jax.random.fold_in(jax.random.fold_in(own_key, 6), dim), (blocks,), jnp.float32, least / len(pieces), high / len(pieces))
        return jnp.repeat(jnp.exp(draws), shape[dim] // blocks).reshape((-1,) + (1,) * (len(shape) - dim - 1))

    factor_of = one(*pieces[0])
    for cut in pieces[1:]:
        factor_of = factor_of * one(*cut)
    return factor_of


def gaussian(key, dims, width, reach, cuts=(), kind=jnp.bfloat16):
    level = block_scale(key, dims, cuts, -0.22, 0.18) if cuts else 1.0
    array = jax.random.normal(key, dims, jnp.float32) * width * level
    return jnp.minimum(jnp.maximum(array, -reach), reach).astype(kind)


def setup_inputs(seed: int = 0) -> dict:
    key_of = jax.random.split(jax.random.key(seed), 9)
    logits = draw_logits(jax.random.fold_in(key_of[8], 71), 0)
    targets = touch_ends(jax.random.randint(key_of[1], (TOKENS,), 0, VOCAB), jax.random.fold_in(key_of[1], 1), 0, VOCAB - 1).astype(jnp.int32)
    resp_mask = draw_resp_mask(jax.random.fold_in(key_of[8], 71), 0)
    rewards = touch_ends(jax.random.randint(key_of[3], (SEQS,), 0, 11), jax.random.fold_in(key_of[3], 1), 0, 10).astype(jnp.int32)
    groups = draw_groups(jax.random.fold_in(key_of[8], 71), 0)
    unit_grad = gaussian(key_of[5], (TOKENS, D), 32.0, 192.0, ((0, 32),))
    mix = gaussian(key_of[6], (TOKENS, QW), 1.0, 6.0, ((0, 8), (1, 4)))
    w_out = gaussian(key_of[7], (QW, D), QW ** -0.5, 0.125, ((0, 4), (1, 8)))
    return {"logits": logits, "targets": targets, "resp_mask": resp_mask, "rewards": rewards, "groups": groups, "unit_grad": unit_grad, "mix": mix, "w_out": w_out}


def sample_logprob(inputs):
    values, chosen = inputs
    wide = values.astype(jnp.float32)
    highest = jnp.max(wide, axis=1)
    summed = jnp.sum(jnp.exp(wide - highest[:, None]), axis=1)
    picked = jnp.take_along_axis(wide, chosen[:, None].astype(jnp.int32), axis=1)[:, 0]
    return picked - (highest + jnp.log(summed))


def reference(logits, targets, resp_mask, rewards, groups, unit_grad, mix, w_out):
    logprob = lax.map(sample_logprob, (logits.reshape(SEQS, ROWS, VOCAB), targets.reshape(SEQS, ROWS)))
    mask_float = resp_mask.astype(jnp.float32).reshape(SEQS, ROWS)
    token_count = jnp.sum(mask_float)
    reward_float = rewards.astype(jnp.float32)
    member = (groups[:, None] == jnp.arange(PROMPTS, dtype=jnp.int32)[None, :]).astype(jnp.float32)
    group_total = jnp.sum(member * reward_float[:, None], axis=0)
    own_total = jnp.sum(member * group_total[None, :], axis=1)
    advantage = reward_float - (own_total - reward_float) / (K - 1)
    weight = advantage[:, None] * mask_float / token_count
    policy_loss = -jnp.sum(weight * logprob)
    grad_out = (-weight.reshape(TOKENS)[:, None] * unit_grad.astype(jnp.float32)).astype(jnp.bfloat16)
    grad_mix = jnp.dot(grad_out, w_out.T, preferred_element_type=jnp.float32).astype(jnp.bfloat16)
    grad_w_out = jnp.dot(mix.T, grad_out, preferred_element_type=jnp.float32).astype(jnp.bfloat16)
    return logprob.reshape(TOKENS), policy_loss, grad_mix, grad_w_out
```

```python
import functools

import jax
import jax.numpy as jnp
from jax import lax
from jax.experimental import pallas as pl
from jax.experimental.pallas import tpu as pltpu
from jax.sharding import PartitionSpec as P

K = 4
CORES = 2
PAIR = 2
MESH = pl.DeviceIdType.MESH
F32 = jnp.float32
BF16 = jnp.bfloat16


def kernel(
    nd, nm, ug, lg, w, mix, pk, lp_out, loss_out, gm_out, gw_out,
    gbuf, gwt, mixb, mixt, lgv, wv, pkb, lseb, lossb, ysend, yrecv, zsend, zrecv,
    loc, g1, gx, gc, pks, lses, losss, mz, my, ry, rz,
):
    A = nd // PAIR
    X = nm // CORES
    d = lax.axis_index("dp")
    m = lax.axis_index("mp")
    a, b = d // PAIR, lax.rem(d, PAIR)
    x, c = m // CORES, lax.rem(m, CORES)
    rows = ug.shape[0]
    tok, vocab = lg.shape
    cols = w.shape[1]

    def split(k):
        if isinstance(k, int):
            return (k % A + 1) % A, (1 if k < A else 0)
        return lax.rem(lax.rem(k, A) + 1, A), 1 - k // A

    def dest(k):
        oa, ob = split(k)
        return lax.rem(a + oa, A) * PAIR + lax.rem(b + ob, PAIR)

    def origin(k):
        oa, ob = split(k)
        return lax.rem(a - oa + A, A) * PAIR + lax.rem(b + ob, PAIR)

    def remote(src, dst, sems, idx, dd, mm):
        return pltpu.make_async_remote_copy(
            src_ref=src, dst_ref=dst, send_sem=sems.at[(0,) + idx], recv_sem=sems.at[(1,) + idx],
            device_id=(dd, mm), device_id_type=MESH,
        )

    other_b = a * PAIR + (1 - b)
    core_m = x * CORES + (1 - c)

    locals_ = [
        pltpu.make_async_copy(lg, lgv, loc.at[0]),
        pltpu.make_async_copy(pk, pkb.at[d], loc.at[1]),
        pltpu.make_async_copy(w, wv, loc.at[2]),
        pltpu.make_async_copy(mix, mixb.at[d], loc.at[3]),
        pltpu.make_async_copy(ug.at[:, pl.ds(pl.multiple_of(d * cols, 128), cols)], gbuf.at[d, m], loc.at[4]),
    ]
    for cp in locals_:
        cp.start()

    barrier = pltpu.get_barrier_semaphore()
    for k in range(nd - 1):
        pl.semaphore_signal(barrier, inc=1, device_id=(dest(k), m), device_id_type=MESH)
    for j in range(1, nm):
        pl.semaphore_signal(barrier, inc=1, device_id=(d, lax.rem(m + j, nm)), device_id_type=MESH)
    pl.semaphore_wait(barrier, nd + nm - 2)

    g1c = []
    for k in range(nd - 1):
        t = dest(k)
        cp = remote(
            ug.at[:, pl.ds(pl.multiple_of(t * cols, 128), cols)], gbuf.at[d, m], g1, (k,), t, m
        )
        cp.start()
        g1c.append(cp)
    own = ug.at[:, pl.ds(pl.multiple_of(d * cols, 128), cols)]

    def xcopy(xo, k, src=None):
        s = origin(k)
        return remote(
            gbuf.at[s, m] if src is None else src, gbuf.at[s, m], gx, (xo, k), d,
            lax.rem(x + xo, X) * CORES + c,
        )

    def ccopy(xo, k, src=None):
        s = origin(k)
        slot = gbuf.at[s, lax.rem(x - xo + X, X) * CORES + c]
        return remote(slot if src is None else src, slot, gc, (xo, k), d, core_m)

    last = nd - 1
    for xo in range(1, X):
        xcopy(xo, last, own).start()
    ccopy(0, last, own).start()
    pkc = []
    for k in range(nd - 1):
        cp = remote(pk, pkb.at[d], pks, (k,), dest(k), m)
        cp.start()
        pkc.append(cp)

    def mzcopy(oa):
        return remote(mix, mixb.at[d], mz, (oa,), lax.rem(a + oa, A) * PAIR + b, m)

    def mycopy(oa):
        s = lax.rem(a - oa + A, A) * PAIR + b
        slot = mixb.at[s]
        return remote(mix if oa == 0 else slot, slot, my, (oa,), other_b, m)

    for oa in range(1, A):
        mzcopy(oa).start()
    mycopy(0).start()

    eye = lax.broadcasted_iota(jnp.int32, (tok, tok), 0) == lax.broadcasted_iota(jnp.int32, (tok, tok), 1)

    def to_col(row):
        return jnp.sum(jnp.where(eye, row, 0.0), axis=1, keepdims=True)

    def to_row(col):
        return jnp.sum(jnp.where(eye, col, 0.0), axis=0, keepdims=True)

    locals_[0].wait()
    locals_[1].wait()
    lane = lax.broadcasted_iota(jnp.int32, (tok, 128), 1).astype(F32)
    own_pack = pkb[d]
    target = to_col(own_pack[3:4]) - (m * vocab).astype(F32)

    def part(j):
        return lgv[:, pl.ds(pl.multiple_of(j * 128, 128), 128)].astype(F32)

    steps = vocab // 128
    top = lax.fori_loop(1, steps, lambda j, acc: jnp.maximum(acc, part(j)), part(0))
    top = jnp.max(top, axis=1, keepdims=True)

    def sums(j, carry):
        tot, pick = carry
        v = part(j)
        hit = lane + (j * 128).astype(F32) == target
        return tot + jnp.exp(v - top), pick + jnp.where(hit, v, 0.0)

    zero = jnp.zeros((tok, 128), F32)
    tot, pick = lax.fori_loop(0, steps, sums, (zero, zero))
    tot = jnp.sum(tot, axis=1, keepdims=True)
    pick = jnp.sum(pick, axis=1, keepdims=True)
    sub = lax.broadcasted_iota(jnp.int32, (8, tok), 0)
    lseb[m] = jnp.where(sub == 0, to_row(top), jnp.where(sub == 1, to_row(tot), to_row(pick)))
    lsec = []

    def forward(k):
        g1c[k].wait_recv()
        for xo in range(1, X):
            xcopy(xo, k).start()
        ccopy(0, k).start()

    def forward_x(k):
        for xo in range(1, X):
            xcopy(xo, k).wait_recv()
            ccopy(xo, k).start()

    forward(0)
    for j in range(1, nm):
        cp = remote(lseb.at[m], lseb.at[m], lses, (j,), d, lax.rem(m + j, nm))
        cp.start()
        lsec.append(cp)
    forward_x(last)
    for k in range(1, nd - 1):
        forward(k)
        forward_x(k - 1)
    for cp in pkc:
        cp.wait_recv()
    packs = pkb[...]
    masks = packs[:, 0:1, :]
    count = jnp.sum(jnp.sum(masks, axis=0), axis=1, keepdims=True)

    def weight_row(s):
        p = pkb[s]
        reward = p[1:2]
        total = jnp.sum(jnp.where(packs[:, 2:3, :] == p[2:3][None], packs[:, 1:2, :], 0.0), axis=0)
        advantage = reward - (total - reward) / (K - 1)
        return advantage * p[0:1] / count

    for cp in lsec:
        cp.wait_recv()
    stats = lseb[...]
    high = jnp.max(stats[:, 0:1, :], axis=0)
    summed = jnp.sum(stats[:, 1:2, :] * jnp.exp(stats[:, 0:1, :] - high[None]), axis=0)
    logprob = jnp.sum(stats[:, 2:3, :], axis=0) - (high + jnp.log(summed))
    lp_out[...] = logprob
    share = jnp.sum(weight_row(d) * logprob, axis=1, keepdims=True)
    lossb[d] = jnp.broadcast_to(share, (8, 128))

    forward_x(nd - 2)
    locals_[2].wait()
    locals_[4].wait()

    def partial(k):
        s = origin(k)
        col = to_col(weight_row(s))
        g = gbuf[s].astype(F32).reshape(tok, cols)
        out = (-col * g).astype(BF16)
        gwt[pl.ds(pl.multiple_of(s * tok, tok), tok), :] = out
        return lax.dot_general(out, wv[...], (((1,), (1,)), ((), ())), preferred_element_type=F32)

    def wait_core(k):
        s = origin(k)
        for xo in range(X):
            slot = gbuf.at[s, lax.rem(x - xo + X, X) * CORES + (1 - c)]
            remote(slot, slot, gc, (xo, k), d, core_m).wait_recv()

    def rycopy(k):
        return remote(ysend.at[k], yrecv.at[k], ry, (k,), other_b, m)

    def rzcopy(k):
        oa, _ = split(k)
        return remote(zsend.at[k], zrecv.at[k], rz, (k,), lax.rem(a - oa + A, A) * PAIR + b, m)

    def pair_step(k, carry):
        wait_core(k)
        ysend[k] = partial(k).astype(BF16)
        rycopy(k).start()
        return carry

    lax.fori_loop(0, A, pair_step, 0)
    lossc = []
    for k in range(nd - 1):
        cp = remote(lossb.at[d], lossb.at[d], losss, (k,), dest(k), m)
        cp.start()
        lossc.append(cp)
    locals_[3].wait()
    for oa in range(1, A):
        mzcopy(oa).wait_recv()
        mycopy(oa).start()

    def line_step(k, carry):
        wait_core(A + k)
        p = partial(A + k)
        rycopy(k).wait_recv()
        zsend[k] = (p + yrecv[k].astype(F32)).astype(BF16)
        rzcopy(k).start()
        return carry

    lax.fori_loop(0, A - 1, line_step, 0)
    wait_core(last)
    total = partial(last)
    rycopy(A - 1).wait_recv()
    total = total + yrecv[A - 1].astype(F32)

    def transpose(s):
        mixt[:, pl.ds(pl.multiple_of(s * tok, tok), tok)] = mixb[s].T

    def same_b(oa, carry):
        transpose(lax.rem(a - oa + A, A) * PAIR + b)
        return carry

    def across(oa, carry):
        s = lax.rem(a - oa + A, A) * PAIR + (1 - b)
        remote(mixb.at[s], mixb.at[s], my, (oa,), other_b, m).wait_recv()
        transpose(s)
        return carry

    lax.fori_loop(0, A, same_b, 0)
    lax.fori_loop(0, A, across, 0)
    width = 256

    def product(j, carry):
        at = pl.ds(pl.multiple_of(j * width, width), width)
        gw_out[:, at] = jnp.dot(mixt[...], gwt[:, at], preferred_element_type=F32).astype(BF16)
        return carry

    lax.fori_loop(0, cols // width, product, 0)
    for k in range(A - 1):
        rzcopy(k).wait_recv()
        total = total + zrecv[k].astype(F32)
    gm_out[...] = total.astype(BF16)
    for cp in lossc:
        cp.wait_recv()
    loss_out[0, 0] = -jnp.sum(jnp.sum(lossb[...][:, 0:1, 0:1], axis=0))

    for cp in g1c + pkc + lsec + lossc:
        cp.wait_send()
    for k in range(nd):
        for xo in range(X):
            ccopy(xo, k).wait_send()
            if xo:
                xcopy(xo, k).wait_send()
    for oa in range(A):
        mycopy(oa).wait_send()
        rycopy(oa).wait_send()
        if oa:
            mzcopy(oa).wait_send()
            rzcopy(oa - 1).wait_send()


def solution(mesh):
    nd, nm = mesh.shape["dp"], mesh.shape["mp"]
    A, X = nd // PAIR, nm // CORES

    def shards(logits, targets, resp_mask, rewards, groups, unit_grad, mix, w_out):
        tok, vocab = logits.shape
        rows = unit_grad.shape[0]
        heads, cols = w_out.shape
        pack = jnp.stack(
            [
                resp_mask.astype(F32),
                jnp.broadcast_to(rewards.astype(F32), (tok,)),
                jnp.broadcast_to(groups.astype(F32), (tok,)),
                targets.astype(F32),
            ]
            + [jnp.zeros((tok,), F32)] * 4
        )
        anys = pl.BlockSpec(memory_space=pl.ANY)
        vmem = pl.BlockSpec(memory_space=pltpu.VMEM)
        dma = pltpu.SemaphoreType.DMA
        lp, loss, gm, gw = pl.pallas_call(
            functools.partial(kernel, nd, nm),
            out_shape=(
                jax.ShapeDtypeStruct((1, tok), F32),
                jax.ShapeDtypeStruct((1, 1), F32),
                jax.ShapeDtypeStruct((tok, heads), BF16),
                jax.ShapeDtypeStruct((heads, cols), BF16),
            ),
            in_specs=[anys] * 5,
            out_specs=(vmem, pl.BlockSpec(memory_space=pltpu.SMEM), vmem, vmem),
            scratch_shapes=[
                pltpu.VMEM((nd, nm, rows, cols), BF16),
                pltpu.VMEM((nd * tok, cols), BF16),
                pltpu.VMEM((nd, tok, heads), BF16),
                pltpu.VMEM((heads, nd * tok), BF16),
                pltpu.VMEM((tok, vocab), BF16),
                pltpu.VMEM((heads, cols), BF16),
                pltpu.VMEM((nd, 8, tok), F32),
                pltpu.VMEM((nm, 8, tok), F32),
                pltpu.VMEM((nd, 8, 128), F32),
            ]
            + [pltpu.VMEM((A, tok, heads), BF16)] * 4
            + [
                dma((5,)),
                dma((2, nd)),
                dma((2, X, nd)),
                dma((2, X, nd)),
                dma((2, nd)),
                dma((2, nm)),
                dma((2, nd)),
                dma((2, A)),
                dma((2, A)),
                dma((2, A)),
                dma((2, A)),
            ],
            compiler_params=pltpu.CompilerParams(
                collective_id=0, has_side_effects=True, vmem_limit_bytes=60000 * 1024
            ),
        )(unit_grad, logits, w_out, mix, pack)
        return lp.reshape(tok), loss.reshape(()), gm, gw

    return jax.shard_map(
        shards,
        mesh=mesh,
        in_specs=(
            P("dp", "mp"),
            P("dp"),
            P("dp"),
            P("dp"),
            P("dp"),
            P(("dp", "mp"), None),
            P("dp", "mp"),
            P("mp", "dp"),
        ),
        out_specs=(P("dp"), P(), P("dp", "mp"), P("mp", "dp")),
        check_vma=False,
    )
```

```python
import functools

import jax
import jax.numpy as jnp
from jax import lax
from jax.experimental import pallas as pl
from jax.experimental.pallas import tpu as pltpu
from jax.sharding import PartitionSpec as P

K = 4
CORES = 2
PAIR = 2
MESH = pl.DeviceIdType.MESH
F32 = jnp.float32
BF16 = jnp.bfloat16


def kernel(
    nd, nm, ug, lg, w, mix, pk, lp_out, loss_out, gm_out, gw_out,
    gbuf, gwt, mixb, mixt, lgv, wv, pkb, lseb, lossb, ysend, yrecv, zsend, zrecv,
    loc, g1, gx, gc, pks, lses, losss, mz, my, ry, rz,
):
    A = nd // PAIR
    X = nm // CORES
    d = lax.axis_index("dp")
    m = lax.axis_index("mp")
    a, b = d // PAIR, lax.rem(d, PAIR)
    x, c = m // CORES, lax.rem(m, CORES)
    rows = ug.shape[0]
    tok, vocab = lg.shape
    cols = w.shape[1]

    def split(k):
        if isinstance(k, int):
            return (k % A + 1) % A, (1 if k < A else 0)
        return lax.rem(lax.rem(k, A) + 1, A), 1 - k // A

    def dest(k):
        oa, ob = split(k)
        return lax.rem(a + oa, A) * PAIR + lax.rem(b + ob, PAIR)

    def origin(k):
        oa, ob = split(k)
        return lax.rem(a - oa + A, A) * PAIR + lax.rem(b + ob, PAIR)

    def remote(src, dst, sems, idx, dd, mm):
        return pltpu.make_async_remote_copy(
            src_ref=src, dst_ref=dst, send_sem=sems.at[(0,) + idx], recv_sem=sems.at[(1,) + idx],
            device_id=(dd, mm), device_id_type=MESH,
        )

    other_b = a * PAIR + (1 - b)
    core_m = x * CORES + (1 - c)

    locals_ = [
        pltpu.make_async_copy(lg, lgv, loc.at[0]),
        pltpu.make_async_copy(pk, pkb.at[d], loc.at[1]),
        pltpu.make_async_copy(w, wv, loc.at[2]),
        pltpu.make_async_copy(mix, mixb.at[d], loc.at[3]),
        pltpu.make_async_copy(ug.at[:, pl.ds(pl.multiple_of(d * cols, 128), cols)], gbuf.at[d, m], loc.at[4]),
    ]
    for cp in locals_:
        cp.start()

    barrier = pltpu.get_barrier_semaphore()
    for k in range(nd - 1):
        pl.semaphore_signal(barrier, inc=1, device_id=(dest(k), m), device_id_type=MESH)
    for j in range(1, nm):
        pl.semaphore_signal(barrier, inc=1, device_id=(d, lax.rem(m + j, nm)), device_id_type=MESH)
    pl.semaphore_wait(barrier, nd + nm - 2)

    pkc = []
    for k in range(nd - 1):
        cp = remote(pk, pkb.at[d], pks, (k,), dest(k), m)
        cp.start()
        pkc.append(cp)

    g1c = []
    for k in range(nd - 1):
        t = dest(k)
        cp = remote(
            ug.at[:, pl.ds(pl.multiple_of(t * cols, 128), cols)], gbuf.at[d, m], g1, (k,), t, m
        )
        cp.start()
        g1c.append(cp)
    own = ug.at[:, pl.ds(pl.multiple_of(d * cols, 128), cols)]

    def xcopy(xo, k, src=None):
        s = origin(k)
        return remote(
            gbuf.at[s, m] if src is None else src, gbuf.at[s, m], gx, (xo, k), d,
            lax.rem(x + xo, X) * CORES + c,
        )

    def ccopy(xo, k, src=None):
        s = origin(k)
        slot = gbuf.at[s, lax.rem(x - xo + X, X) * CORES + c]
        return remote(slot if src is None else src, slot, gc, (xo, k), d, core_m)

    last = nd - 1
    for xo in range(1, X):
        xcopy(xo, last, own).start()
    ccopy(0, last, own).start()

    def line_copy(way, h, src=None):
        s = a - h * way
        slot = mixb.at[s * PAIR + b]
        return remote(
            slot if src is None else src, slot, mz, ((1 - way) // 2, h),
            (a + way) * PAIR + b, m,
        )

    def hand_on(way, h, src=None):
        s = a - h * way
        slot = mixb.at[s * PAIR + b]
        return remote(
            slot if src is None else src, slot, mz, ((1 - way) // 2, h + 1),
            (a + way) * PAIR + b, m,
        )

    def has_next(way):
        return a < A - 1 if way == 1 else a > 0

    def has_piece(way, h):
        return a >= h if way == 1 else a + h < A

    def my_copy(s, src=None):
        slot = mixb.at[s * PAIR + b]
        return remote(slot if src is None else src, slot, my, (s,), other_b, m)

    for way in (1, -1):

        @pl.when(has_next(way))
        def _():
            hand_on(way, 0, mix).start()

    my_copy(a, mix).start()

    def transpose(s):
        mixt[:, pl.ds(pl.multiple_of(s * tok, tok), tok)] = mixb[s].T

    def mix_step(h):
        for way in (1, -1):

            @pl.when(has_piece(way, h))
            def _():
                line_copy(way, h).wait_recv()

                if h < A - 1:

                    @pl.when(has_next(way))
                    def _():
                        hand_on(way, h).start()

                my_copy(a - h * way).start()
                transpose((a - h * way) * PAIR + b)

    eye = lax.broadcasted_iota(jnp.int32, (tok, tok), 0) == lax.broadcasted_iota(jnp.int32, (tok, tok), 1)

    def to_col(row):
        return jnp.sum(jnp.where(eye, row, 0.0), axis=1, keepdims=True)

    def to_row(col):
        return jnp.sum(jnp.where(eye, col, 0.0), axis=0, keepdims=True)

    locals_[0].wait()
    locals_[1].wait()
    lane = lax.broadcasted_iota(jnp.int32, (tok, 128), 1).astype(F32)
    own_pack = pkb[d]
    target = to_col(own_pack[3:4]) - (m * vocab).astype(F32)

    def part(j):
        return lgv[:, pl.ds(pl.multiple_of(j * 128, 128), 128)].astype(F32)

    steps = vocab // 128
    top = lax.fori_loop(1, steps, lambda j, acc: jnp.maximum(acc, part(j)), part(0))
    top = jnp.max(top, axis=1, keepdims=True)

    def sums(j, carry):
        tot, pick = carry
        v = part(j)
        hit = lane + (j * 128).astype(F32) == target
        return tot + jnp.exp(v - top), pick + jnp.where(hit, v, 0.0)

    zero = jnp.zeros((tok, 128), F32)
    tot, pick = lax.fori_loop(0, steps, sums, (zero, zero))
    tot = jnp.sum(tot, axis=1, keepdims=True)
    pick = jnp.sum(pick, axis=1, keepdims=True)
    sub = lax.broadcasted_iota(jnp.int32, (8, tok), 0)
    lseb[m] = jnp.where(sub == 0, to_row(top), jnp.where(sub == 1, to_row(tot), to_row(pick)))
    lsec = []

    def forward(k):
        g1c[k].wait_recv()
        for xo in range(1, X):
            xcopy(xo, k).start()
        ccopy(0, k).start()

    def forward_x(k):
        for xo in range(1, X):
            xcopy(xo, k).wait_recv()
            ccopy(xo, k).start()

    def wait_core(k):
        s = origin(k)
        for xo in range(X):
            slot = gbuf.at[s, lax.rem(x - xo + X, X) * CORES + (1 - c)]
            remote(slot, slot, gc, (xo, k), d, core_m).wait_recv()

    def rycopy(k):
        return remote(ysend.at[k], yrecv.at[k], ry, (k,), other_b, m)

    def rzcopy(k):
        oa, _ = split(k)
        return remote(zsend.at[k], zrecv.at[k], rz, (k,), lax.rem(a - oa + A, A) * PAIR + b, m)

    for j in range(1, nm):
        cp = remote(lseb.at[m], lseb.at[m], lses, (j,), d, lax.rem(m + j, nm))
        cp.start()
        lsec.append(cp)
    forward_x(last)
    locals_[3].wait()
    transpose(d)
    locals_[2].wait()
    locals_[4].wait()
    for cp in pkc:
        cp.wait_recv()
    packs = pkb[...]
    masks = packs[:, 0:1, :]
    count = jnp.sum(jnp.sum(masks, axis=0), axis=1, keepdims=True)

    def weight_row(s):
        p = pkb[s]
        reward = p[1:2]
        total = jnp.sum(jnp.where(packs[:, 2:3, :] == p[2:3][None], packs[:, 1:2, :], 0.0), axis=0)
        advantage = reward - (total - reward) / (K - 1)
        return advantage * p[0:1] / count

    def partial(k):
        s = origin(k)
        col = to_col(weight_row(s))
        g = gbuf[s].astype(F32).reshape(tok, cols)
        out = (-col * g).astype(BF16)
        gwt[pl.ds(pl.multiple_of(s * tok, tok), tok), :] = out
        return lax.dot_general(out, wv[...], (((1,), (1,)), ((), ())), preferred_element_type=F32)

    def pair_step(k):
        wait_core(k)
        ysend[k] = partial(k).astype(BF16)
        rycopy(k).start()

    def line_step(k):
        wait_core(A + k)
        p = partial(A + k)
        rycopy(k).wait_recv()
        zsend[k] = (p + yrecv[k].astype(F32)).astype(BF16)
        rzcopy(k).start()

    paired = 0
    for k in range(nd - 1):
        forward(k)
        if k >= 1:
            forward_x(k - 1)
        if k >= 2 and paired < A:
            pair_step(paired)
            paired += 1
    forward_x(nd - 2)
    while paired < A:
        pair_step(paired)
        paired += 1
    for h in range(1, A):
        mix_step(h)
        line_step(h - 1)

    for cp in lsec:
        cp.wait_recv()
    stats = lseb[...]
    high = jnp.max(stats[:, 0:1, :], axis=0)
    summed = jnp.sum(stats[:, 1:2, :] * jnp.exp(stats[:, 0:1, :] - high[None]), axis=0)
    logprob = jnp.sum(stats[:, 2:3, :], axis=0) - (high + jnp.log(summed))
    lp_out[...] = logprob
    share = jnp.sum(weight_row(d) * logprob, axis=1, keepdims=True)
    lossb[d] = jnp.broadcast_to(share, (8, 128))
    wait_core(last)
    total = partial(last)
    lossc = []
    for k in range(nd - 1):
        cp = remote(lossb.at[d], lossb.at[d], losss, (k,), dest(k), m)
        cp.start()
        lossc.append(cp)
    rycopy(A - 1).wait_recv()
    total = total + yrecv[A - 1].astype(F32)
    for s in range(A):
        t = s * PAIR + (1 - b)
        remote(mixb.at[t], mixb.at[t], my, (s,), other_b, m).wait_recv()
        transpose(t)
    width = 256

    def product(j, carry):
        at = pl.ds(pl.multiple_of(j * width, width), width)
        gw_out[:, at] = jnp.dot(mixt[...], gwt[:, at], preferred_element_type=F32).astype(BF16)
        return carry

    lax.fori_loop(0, cols // width, product, 0)
    for k in range(A - 1):
        rzcopy(k).wait_recv()
        total = total + zrecv[k].astype(F32)
    gm_out[...] = total.astype(BF16)
    for cp in lossc:
        cp.wait_recv()
    loss_out[0, 0] = -jnp.sum(jnp.sum(lossb[...][:, 0:1, 0:1], axis=0))

    for cp in g1c + pkc + lsec + lossc:
        cp.wait_send()
    for k in range(nd):
        for xo in range(X):
            ccopy(xo, k).wait_send()
            if xo:
                xcopy(xo, k).wait_send()
    for k in range(A):
        my_copy(k).wait_send()
        rycopy(k).wait_send()
        if k < A - 1:
            rzcopy(k).wait_send()
    for way in (1, -1):
        for h in range(A - 1):

            @pl.when(has_next(way) & has_piece(way, h))
            def _():
                hand_on(way, h).wait_send()


def solution(mesh):
    nd, nm = mesh.shape["dp"], mesh.shape["mp"]
    A, X = nd // PAIR, nm // CORES

    def shards(logits, targets, resp_mask, rewards, groups, unit_grad, mix, w_out):
        tok, vocab = logits.shape
        rows = unit_grad.shape[0]
        heads, cols = w_out.shape
        pack = jnp.stack(
            [
                resp_mask.astype(F32),
                jnp.broadcast_to(rewards.astype(F32), (tok,)),
                jnp.broadcast_to(groups.astype(F32), (tok,)),
                targets.astype(F32),
            ]
            + [jnp.zeros((tok,), F32)] * 4
        )
        anys = pl.BlockSpec(memory_space=pl.ANY)
        vmem = pl.BlockSpec(memory_space=pltpu.VMEM)
        dma = pltpu.SemaphoreType.DMA
        lp, loss, gm, gw = pl.pallas_call(
            functools.partial(kernel, nd, nm),
            out_shape=(
                jax.ShapeDtypeStruct((1, tok), F32),
                jax.ShapeDtypeStruct((1, 1), F32),
                jax.ShapeDtypeStruct((tok, heads), BF16),
                jax.ShapeDtypeStruct((heads, cols), BF16),
            ),
            in_specs=[anys] * 5,
            out_specs=(vmem, pl.BlockSpec(memory_space=pltpu.SMEM), vmem, vmem),
            scratch_shapes=[
                pltpu.VMEM((nd, nm, rows, cols), BF16),
                pltpu.VMEM((nd * tok, cols), BF16),
                pltpu.VMEM((nd, tok, heads), BF16),
                pltpu.VMEM((heads, nd * tok), BF16),
                pltpu.VMEM((tok, vocab), BF16),
                pltpu.VMEM((heads, cols), BF16),
                pltpu.VMEM((nd, 8, tok), F32),
                pltpu.VMEM((nm, 8, tok), F32),
                pltpu.VMEM((nd, 8, 128), F32),
            ]
            + [pltpu.VMEM((A, tok, heads), BF16)] * 4
            + [
                dma((5,)),
                dma((2, nd)),
                dma((2, X, nd)),
                dma((2, X, nd)),
                dma((2, nd)),
                dma((2, nm)),
                dma((2, nd)),
                dma((2, 2, A)),
                dma((2, A)),
                dma((2, A)),
                dma((2, A)),
            ],
            compiler_params=pltpu.CompilerParams(
                collective_id=0, has_side_effects=True, vmem_limit_bytes=54000 * 1024
            ),
        )(unit_grad, logits, w_out, mix, pack)
        return lp.reshape(tok), loss.reshape(()), gm, gw

    return jax.shard_map(
        shards,
        mesh=mesh,
        in_specs=(
            P("dp", "mp"),
            P("dp"),
            P("dp"),
            P("dp"),
            P("dp"),
            P(("dp", "mp"), None),
            P("dp", "mp"),
            P("mp", "dp"),
        ),
        out_specs=(P("dp"), P(), P("dp", "mp"), P("mp", "dp")),
        check_vma=False,
    )
```
